32 devices in a mesh: gx: 4 (over z), gy: 4 (over y, core), gz: 2 (over x).
Axes of the slice: x: 2, y: 2, z: 4, core: 2. Of those that a mesh axis runs over, the one named last changes fastest.
Arguments:
- positions_now: float32 [32, 16, 2, 4, 128], P('gx', 'gy', 'gz'), may hold values from 0 to 1
- velocities: float32 [32, 16, 2, 3, 128], P('gx', 'gy', 'gz'), may hold values from -6 to 6
- positions_next: float32 [32, 16, 2, 3, 128], P('gx', 'gy', 'gz'), may hold values from 0 to 1
- halo_counts: int32 [32, 16, 2], P('gx', 'gy', 'gz'), may hold values from 1 to 128, as said below
- neighbour_lists: int32 [32, 16, 2, 14], P('gx', 'gy', 'gz'), may hold values from 0 to 26, as said below
- descendants: int32 [32, 16, 2, 2, 128], P('gx', 'gy', 'gz'), may hold values from 0 to 127, as said below
Outputs:
- drift: float32 [32, 16, 2, 3, 128], P('gx', 'gy', 'gz')
- tension: float32 [32, 16, 2, 128], P('gx', 'gy', 'gz')
The draws below stay inside these ranges and needn't reach their ends.
Inputs may be any that keep to these rules, and one draw needn't show every extreme that they name: `halo_counts`: every cell holds 1 to 128 live halos; some cell holds exactly 128. `neighbour_lists`: each cell's list begins with code 13 (the cell itself) and holds distinct codes. `descendants`: row 0 is a code 0 to 26; row 1 is a live slot of the descendant's cell.
All inputs are finite; a program needn't handle non-finite values.
Results may differ from the reference program's by a relative error of at most 0.0003.
Values sent between devices are 32-bit elements; how exact they have to be, the bound alone decides.
A program may use at most 64 MiB of HBM per device.

```python
import jax
import jax.numpy as jnp
from jax import lax

SLOTS = 128
NBR = 14
NX = 32
NY = 16
NZ = 2


def make_counts(key):
    shape = (NX, NY, NZ)
    xpos = jnp.arange(NX, dtype=jnp.int32)[:, None, None]
    upper = 32 + 96 * (xpos + 1) // NX
    raw = jax.random.randint(key, shape, 0, 1 << 20, dtype=jnp.int32)
    counts = 1 + raw % upper
    return counts.at[NX - 1, 0, 0].set(SLOTS)


def draw_halo_counts(key, part):
    return make_counts(jax.random.fold_in(key, 11))


def draw_neighbour_lists(key, part):
    sub = jax.random.fold_in(key, 23)
    scores = jax.random.randint(sub, (NX, NY, NZ, 26), 0, 1 << 20, dtype=jnp.int32) * 32 + jnp.arange(26, dtype=jnp.int32)
    order = jnp.argsort(scores, axis=-1, stable=True)[..., :NBR - 1].astype(jnp.int32)
    codes = jnp.where(order < 13, order, order + 1)
    selfcode = jnp.full((NX, NY, NZ, 1), 13, jnp.int32)
    return jnp.concatenate([selfcode, codes], axis=-1)


def draw_descendants(key, part):
    counts = make_counts(jax.random.fold_in(key, 11))
    sub = jax.random.fold_in(key, 37)
    first, second = jax.random.split(sub)
    codes = jax.random.randint(first, (NX, NY, NZ, SLOTS), 0, 27, dtype=jnp.int32)
    rolled = []
    for code in range(27):
        dx, dy, dz = (code // 9 - 1, code // 3 % 3 - 1, code % 3 - 1)
        rolled.append(jnp.roll(counts, (-dx, -dy, -dz), axis=(0, 1, 2)))
    table = jnp.stack(rolled, axis=-1)
    hits = (codes[..., None] == jnp.arange(27, dtype=jnp.int32)).astype(jnp.int32)
    target_count = jnp.sum(hits * table[:, :, :, None, :], axis=-1)
    raw = jax.random.randint(second, (NX, NY, NZ, SLOTS), 0, 1 << 20, dtype=jnp.int32)
    slotid = raw % target_count
    return jnp.stack([codes, slotid], axis=3)


def shard_levels(rng, extent, pieces, low, largest):
    loudness = 1.0
    for position, parts in pieces:
        heights = jax.random.uniform(jax.random.fold_in(jax.random.fold_in(rng, 6), position), (parts,), jnp.float32, low / len(pieces), largest / len(pieces))
        loudness = loudness * jnp.repeat(jnp.exp(heights), extent[position] // parts).reshape((-1,) + (1,) * (len(extent) - 1 - position))
    return loudness


def noise(own_key, shape, scale, limit, cuts=(), kind=jnp.bfloat16):
    result = scale * jax.random.normal(own_key, shape, jnp.float32)
    if cuts:
        result = result * shard_levels(own_key, shape, cuts, -0.22, 0.18)
    return jnp.clip(result, -limit, limit).astype(kind)


def setup_inputs(seed: int = 0) -> dict:
    splits = jax.random.split(jax.random.key(seed), 7)
    positions_now = jnp.clip(1.0 * jax.random.uniform(splits[0], (NX, NY, NZ, 4, SLOTS), jnp.float32) ** shard_levels(splits[0], (NX, NY, NZ, 4, SLOTS), ((0, 4), (1, 4), (2, 2)), -0.2, 0.2), 0.0, 1.0)
    velocities = noise(splits[1], (NX, NY, NZ, 3, SLOTS), 1.0, 6.0, ((0, 4), (1, 4), (2, 2)), jnp.float32)
    positions_next = jnp.clip(1.0 * jax.random.uniform(splits[2], (NX, NY, NZ, 3, SLOTS), jnp.float32) ** shard_levels(splits[2], (NX, NY, NZ, 3, SLOTS), ((0, 4), (1, 4), (2, 2)), -0.2, 0.2), 0.0, 1.0)
    halo_counts = draw_halo_counts(jax.random.fold_in(splits[6], 71), 0)
    neighbour_lists = draw_neighbour_lists(jax.random.fold_in(splits[6], 71), 0)
    descendants = draw_descendants(jax.random.fold_in(splits[6], 71), 0)
    return {"positions_now": positions_now, "velocities": velocities, "positions_next": positions_next, "halo_counts": halo_counts, "neighbour_lists": neighbour_lists, "descendants": descendants}


EPS_SQ = 0.01
STEP_DT = 0.3
HALF_KICK = 0.045

def offsets_of(code):
    return (code // 9 - 1, code // 3 % 3 - 1, code % 3 - 1)

def stack_state(positions_now, positions_next, halo_counts):
    slots = positions_now.shape[-1]
    live = (jnp.arange(slots, dtype=jnp.int32)[None, None, None, :] < halo_counts[..., None]).astype(jnp.float32)
    masses = positions_now[:, :, :, 3:4, :] * live[:, :, :, None, :]
    return (jnp.concatenate([positions_now[:, :, :, :3, :], masses, positions_next], axis=3), live)

def predict(padded, neighbour_lists, velocities, descendants, halo_counts):
    cx, cy, cz = neighbour_lists.shape[:3]
    width = neighbour_lists.shape[3]
    px, py, pz = (cx + 2, cy + 2, cz + 2)
    slots = padded.shape[-1]
    cells = cx * cy * cz
    flat = padded.reshape(px * py * pz, 7, slots)
    next_rows = jnp.transpose(flat[:, 4:7, :], (0, 2, 1)).reshape(px * py * pz * slots, 3)
    grid = jnp.indices((cx, cy, cz), dtype=jnp.int32).reshape(3, cells)
    base = ((grid[0] + 1) * py + grid[1] + 1) * pz + grid[2] + 1
    group = 32 if cells % 32 == 0 else cells
    blocks = cells // group
    lists = neighbour_lists.reshape(blocks, group, width)
    vel = velocities.reshape(blocks, group, 3, slots)
    desc = descendants.reshape(blocks, group, 2, slots)
    counts = halo_counts.reshape(blocks, group)
    bases = base.reshape(blocks, group)

    def one_group(items):
        base_g, list_g, vel_g, desc_g, count_g = items
        own = flat[base_g]
        pos = own[:, :3, :]

        def step(accel, code):
            dx, dy, dz = offsets_of(code)
            source = flat[base_g + dx * py * pz + dy * pz + dz]
            offset = jnp.stack([dx, dy, dz], 1).astype(jnp.float32)
            spot = offset[:, :, None] + source[:, :3, :]
            diff = spot[:, :, None, :] - pos[:, :, :, None]
            dist_sq = lax.optimization_barrier(jnp.sum(diff * diff, axis=1)) + EPS_SQ
            weight = source[:, 3, None, :] / (dist_sq * jnp.sqrt(dist_sq))
            return (accel + lax.optimization_barrier(jnp.sum(diff * weight[:, None, :, :], axis=3)), None)
        accel, _ = lax.scan(step, jnp.zeros(pos.shape, jnp.float32), jnp.transpose(list_g))
        predicted = pos + STEP_DT * vel_g + HALF_KICK * accel
        dcode = desc_g[:, 0, :]
        dslot = desc_g[:, 1, :]
        ddx, ddy, ddz = offsets_of(dcode)
        target = base_g[:, None] + ddx * py * pz + ddy * pz + ddz
        found = jnp.transpose(next_rows[target * slots + dslot], (0, 2, 1))
        offset = jnp.stack([ddx, ddy, ddz], 1).astype(jnp.float32)
        error = offset + found - predicted
        live = (jnp.arange(slots, dtype=jnp.int32)[None, :] < count_g[:, None]).astype(jnp.float32)
        drift = error * live[:, None, :]
        squared = lax.optimization_barrier(jnp.sum(error * error, axis=1)) * live
        return (drift, squared)
    drift, squared = lax.map(one_group, (bases, lists, vel, desc, counts))
    return (drift.reshape(cx, cy, cz, 3, slots), squared.reshape(cx, cy, cz, slots))

def reference(positions_now, velocities, positions_next, halo_counts, neighbour_lists, descendants):
    state, live = stack_state(positions_now, positions_next, halo_counts)
    padded = jnp.pad(state, ((1, 1), (1, 1), (1, 1), (0, 0), (0, 0)), mode='wrap')
    drift, squared = predict(padded, neighbour_lists, velocities, descendants, halo_counts)
    mean_sq = jnp.sum(squared) / jnp.sum(live)
    return (drift, squared / (mean_sq + 1e-06))
```

```python
import functools

import jax
import jax.numpy as jnp
from jax import lax
from jax.experimental import pallas as pl
from jax.experimental.pallas import tpu as pltpu
from jax.sharding import PartitionSpec as P

EPS_SQ = 0.01
STEP_DT = 0.3
HALF_KICK = 0.045
AXES = ("gx", "gy", "gz")
GROUP = 4
MESH = pl.DeviceIdType.MESH


def pieces(tile):
    first = tile.astype(jnp.bfloat16).astype(jnp.float32)
    rest = tile - first
    second = rest.astype(jnp.bfloat16).astype(jnp.float32)
    return first, second, rest - second


def kernel(
    dims, width, sizes, lists, counts, pos_hbm, next_hbm, vel_hbm, desc_hbm, drift_ref, tension_ref,
    pos, nxt, vel, desc, now_pad, next_pad, feats, moms, lhs, squared, stat, inbox,
    load_sems, now_send, now_recv, next_send, next_recv, stat_send, stat_recv,
):
    cx, cy, cz = dims
    sx, sy, sz = sizes
    py, pz = cy + 2, cz + 2
    cells = cx * cy * cz
    slots = pos.shape[-1]
    folded = sz == 2 and cz == 1
    total = sx * sy * sz
    me = tuple(lax.axis_index(name) for name in AXES)
    row8 = lax.broadcasted_iota(jnp.int32, (8, slots), 0)
    row4 = lax.broadcasted_iota(jnp.int32, (4, slots), 0)
    lane4 = lax.broadcasted_iota(jnp.int32, (4, slots), 1)

    loads = [
        pltpu.make_async_copy(src, dst, load_sems.at[i])
        for i, (src, dst) in enumerate(((pos_hbm, pos), (next_hbm, nxt), (vel_hbm, vel), (desc_hbm, desc)))
    ]
    for load in loads:
        load.start()

    def peer(step):
        where = []
        at = step
        for mine, size in zip(reversed(me), reversed(sizes)):
            where.append(lax.rem(mine + at % size, size))
            at = at // size
        return tuple(reversed(where))

    def each_peer(act):
        if total <= 64:
            for step in range(1, total):
                act(step, peer(step))
        else:
            lax.fori_loop(1, total, lambda step, _: (act(step, peer(step)), 0)[1], 0)

    barrier = pltpu.get_barrier_semaphore()
    each_peer(lambda step, who: pl.semaphore_signal(barrier, inc=1, device_id=who, device_id_type=MESH))

    def plane(iz, dz):
        return (1 if dz == 0 else 0) if folded else iz + 1 + dz

    def split(n):
        return n // (cy * cz), n // cz % cy, n % cz

    def shift_of(ix, iy, iz):
        fx = ix.astype(jnp.float32) - (cx + 2) / 2
        fy = iy.astype(jnp.float32) - (cy + 2) / 2
        fz = iz.astype(jnp.float32) - (cz + 2) / 2
        return jnp.where(row4 == 0, fx, jnp.where(row4 == 1, fy, jnp.where(row4 == 2, fz, 0.0)))

    loads[0].wait()
    loads[1].wait()

    def stage(n, _):
        ix, iy, iz = split(n)
        tile = pos[n]
        now_pad[ix + 1, iy + 1, plane(iz, 0)] = jnp.where((row4 == 3) & (lane4 >= counts[iy, iz, ix]), 0.0, tile)
        rows = [nxt[pl.ds(3 * n + r, 1), :] for r in range(3)]
        next_pad[ix + 1, iy + 1, plane(iz, 0)] = jnp.concatenate(rows + [jnp.zeros_like(rows[0])], axis=0)
        return 0

    lax.fori_loop(0, cells, stage, 0, unroll=4)

    def face(d, size):
        if d == 0:
            return pl.ds(1, size), pl.ds(1, size)
        return (pl.ds(size, 1), pl.ds(0, 1)) if d > 0 else (pl.ds(1, 1), pl.ds(size + 1, 1))

    ways = [
        (dx, dy, dz)
        for dz in ((0, 1) if folded else (0, 1, -1))
        for dx in (0, 1, -1)
        for dy in (0, 1, -1)
        if (dx, dy, dz) != (0, 0, 0)
    ]
    ways.sort(key=lambda way: (way[2] == 0, abs(way[0]) + abs(way[1])))

    def exchange(buf, send_sems, recv_sems):
        made = []
        for i, (dx, dy, dz) in enumerate(ways):
            fx, tx = face(dx, cx)
            fy, ty = face(dy, cy)
            if folded:
                fz, tz = pl.ds(1, 1), pl.ds(1 - dz, 1)
            else:
                fz, tz = face(dz, cz)
            who = tuple(lax.rem(mine + d + size, size) for mine, d, size in zip(me, (dx, dy, dz), sizes))
            made.append(
                pltpu.make_async_remote_copy(
                    src_ref=buf.at[fx, fy, fz],
                    dst_ref=buf.at[tx, ty, tz],
                    send_sem=send_sems.at[i],
                    recv_sem=recv_sems.at[i],
                    device_id=who,
                    device_id_type=MESH,
                )
            )
        for copy in made:
            copy.start()
        return made

    pl.semaphore_wait(barrier, total - 1)
    now_copies = exchange(now_pad, now_send, now_recv)
    next_copies = exchange(next_pad, next_send, next_recv)

    def prepare(px, py_, image, at_plane):
        tile = now_pad[px, py_, at_plane]
        spot = tile + shift_of(jnp.int32(px), jnp.int32(py_), jnp.int32(image))
        square = spot * spot
        size = square[0:1] + square[1:2] + square[2:3]
        base = jnp.where(row4 == 3, size, spot)
        full = jnp.concatenate([base, jnp.where(row4 == 0, 1.0, 0.0)], axis=0)
        a, b, c = pieces(full)
        index = (px * py + py_) * pz + image
        feats[index] = jnp.concatenate([a, a, a, b, b, c], axis=0).astype(jnp.bfloat16)
        mass = tile[3:4]
        mom = jnp.where(row4 == 3, mass, spot * mass)
        mom = jnp.concatenate([mom, jnp.zeros_like(mom)], axis=0)
        high = mom.astype(jnp.bfloat16).astype(jnp.float32)
        moms[index] = jnp.concatenate([high, mom - high], axis=0).astype(jnp.bfloat16)
        return spot, size

    def mine(n, _):
        ix, iy, iz = split(n)
        spot, size = prepare(ix + 1, iy + 1, iz + 1, plane(iz, 0))
        base = jnp.where(row4 == 3, 1.0, -2.0 * spot)
        extra = jnp.where(row4 == 0, size + EPS_SQ, 0.0)
        a, b, c = pieces(jnp.concatenate([base, extra], axis=0))
        lhs[n] = jnp.concatenate([a, b, c, a, b, a], axis=0).T.astype(jnp.bfloat16)
        return 0

    lax.fori_loop(0, cells, mine, 0, unroll=4)
    for copy in now_copies:
        copy.wait()

    def rim_x(i, _):
        for px in (0, cx + 1):
            prepare(px, i // cz, i % cz + 1, plane(i % cz, 0))
        return 0

    def rim_y(i, _):
        for py_ in (0, cy + 1):
            prepare(i // cz + 1, py_, i % cz + 1, plane(i % cz, 0))
        return 0

    def rim_z(i, _):
        for image, dz in ((0, -1), (cz + 1, 1)):
            prepare(i // py, i % py, image, plane(0 if dz < 0 else cz - 1, dz))
        return 0

    lax.fori_loop(0, py * cz, rim_x, 0, unroll=2)
    lax.fori_loop(0, cx * cz, rim_y, 0, unroll=2)
    lax.fori_loop(0, (cx + 2) * py, rim_z, 0, unroll=2)
    for copy in next_copies:
        copy.wait()
    loads[2].wait()
    loads[3].wait()

    def pull(n):
        ix, iy, iz = split(n)
        corner = (ix * py + iy) * pz + iz
        sources = []
        for k in range(width):
            code = lists[n, 0, k]
            d9 = (code * 57) >> 9
            d3 = (code * 43) >> 7
            sources.append(corner + d9 * (py * pz) + (d3 - 3 * d9) * pz + code - 3 * d3)
        own = lhs[n]
        acc = jnp.zeros((16, 2 * slots), jnp.float32)
        for k in range(0, width, 2):
            pair = sources[k : k + 2]
            x = jnp.concatenate([feats[s] for s in pair], axis=1)
            z = jnp.concatenate([moms[s] for s in pair], axis=1)
            inv = lax.rsqrt(jnp.dot(own, x, preferred_element_type=jnp.float32))
            weight = inv * inv * inv
            high = weight.astype(jnp.bfloat16)
            low = (weight - high.astype(jnp.float32)).astype(jnp.bfloat16)
            both = jnp.concatenate([high, low], axis=0)
            acc += lax.dot_general(z, both, (((1,), (1,)), ((), ())), preferred_element_type=jnp.float32)
        acc = acc[:, :slots] + acc[:, slots:]
        return acc[0:4] + acc[8:12]

    def target(n, stats):
        ix, iy, iz = split(n)
        sums = pull(n)
        tile = now_pad[ix + 1, iy + 1, plane(iz, 0)]
        accel = sums - (tile + shift_of(ix + 1, iy + 1, iz + 1)) * sums[3:4]
        rows = [vel[pl.ds(3 * n + r, 1), :] for r in range(3)]
        speed = jnp.concatenate(rows + [jnp.zeros_like(rows[0])], axis=0)
        predicted = tile + STEP_DT * speed + HALF_KICK * accel
        links = desc[n]
        dcode = links[0:1]
        d9 = (dcode * 57) >> 9
        d3 = (dcode * 43) >> 7
        dz = dcode - 3 * d3
        d3 = jnp.broadcast_to(d3, (8, slots))
        dslot = jnp.broadcast_to(links[1:2], (8, slots))
        found = [jnp.zeros((8, slots), jnp.float32)] * (1 if folded else 2)
        for c in range(9):
            at = (ix + c // 3, iy + c % 3)
            tiles = [next_pad[at + (plane(iz, d),)] for d in ((-1, 0) if folded else (-1, 0, 1))]
            if not folded:
                tiles.append(jnp.zeros_like(tiles[0]))
            for h in range(len(tiles) // 2):
                got = jnp.take_along_axis(jnp.concatenate(tiles[2 * h : 2 * h + 2], axis=0), dslot, axis=1)
                found[h] = jnp.where(d3 == c, got, found[h])
        if folded:
            there = jnp.where(dz == 1, found[0][4:8], found[0][0:4])
        else:
            there = jnp.where(dz == 1, found[0][4:8], jnp.where(dz == 0, found[0][0:4], found[1][0:4]))
        step = jnp.where(row4 == 0, d9, jnp.where(row4 == 1, d3[0:4] - 3 * d9, dz)).astype(jnp.float32) - 1.0
        live = lane4 < counts[iy, iz, ix]
        error = jnp.where(live & (row4 < 3), step + there - predicted, 0.0)
        for r in range(3):
            drift_ref[pl.ds(3 * n + r, 1), :] = error[r : r + 1]
        summed = jnp.sum(error * error, axis=0, keepdims=True)
        squared[pl.ds(n, 1), :] = summed
        return stats + jnp.where(row8 == 0, summed, jnp.where((row8 == 1) & live[0:1], 1.0, 0.0))

    group = GROUP if cells % GROUP == 0 else 1

    def several(i, stats):
        for u in range(group):
            stats = target(i * group + u, stats)
        return stats

    stats = lax.fori_loop(0, cells // group, several, jnp.zeros((8, slots), jnp.float32))
    stat[...] = stats[0:2]

    def report(step, who):
        pltpu.make_async_remote_copy(
            src_ref=stat,
            dst_ref=inbox.at[step - 1],
            send_sem=stat_send,
            recv_sem=stat_recv,
            device_id=who,
            device_id_type=MESH,
        ).start()

    each_peer(report)
    pltpu.make_async_copy(inbox, inbox, stat_recv).wait()
    sums = stat[...] + jnp.sum(inbox[...], axis=0)
    mean_sq = jnp.sum(sums[0:1], axis=1, keepdims=True) / jnp.sum(sums[1:2], axis=1, keepdims=True)
    tension_ref[...] = squared[...] / (mean_sq + 1e-06)
    pltpu.make_async_copy(inbox, inbox, stat_send).wait()


def shards(positions_now, velocities, positions_next, halo_counts, neighbour_lists, descendants):
    slots = positions_now.shape[-1]
    cx, cy, cz, width = neighbour_lists.shape
    cells = cx * cy * cz
    sizes = tuple(lax.axis_size(name) for name in AXES)
    folded = sizes[2] == 2 and cz == 1
    planes = 2 if folded else cz + 2
    padded = (cx + 2) * (cy + 2) * (cz + 2)
    ways = 17 if folded else 26
    peers = sizes[0] * sizes[1] * sizes[2] - 1

    def rows(array):
        return jnp.transpose(array, (0, 1, 2, 3, 4)).reshape(cells * 3, slots)

    drift, tension = pl.pallas_call(
        functools.partial(kernel, (cx, cy, cz), width, sizes),
        out_shape=(
            jax.ShapeDtypeStruct((cells * 3, slots), jnp.float32),
            jax.ShapeDtypeStruct((cells, slots), jnp.float32),
        ),
        in_specs=[pl.BlockSpec(memory_space=pltpu.SMEM)] * 2 + [pl.BlockSpec(memory_space=pl.ANY)] * 4,
        out_specs=(pl.BlockSpec(memory_space=pltpu.VMEM),) * 2,
        scratch_shapes=[
            pltpu.VMEM((cells, 4, slots), jnp.float32),
            pltpu.VMEM((cells * 3, slots), jnp.float32),
            pltpu.VMEM((cells * 3, slots), jnp.float32),
            pltpu.VMEM((cells, 2, slots), jnp.int32),
            pltpu.VMEM((cx + 2, cy + 2, planes, 4, slots), jnp.float32),
            pltpu.VMEM((cx + 2, cy + 2, planes, 4, slots), jnp.float32),
            pltpu.VMEM((padded, 48, slots), jnp.bfloat16),
            pltpu.VMEM((padded, 16, slots), jnp.bfloat16),
            pltpu.VMEM((cells, slots, 48), jnp.bfloat16),
            pltpu.VMEM((cells, slots), jnp.float32),
            pltpu.VMEM((2, slots), jnp.float32),
            pltpu.VMEM((peers, 2, slots), jnp.float32),
            pltpu.SemaphoreType.DMA((4,)),
            pltpu.SemaphoreType.DMA((ways,)),
            pltpu.SemaphoreType.DMA((ways,)),
            pltpu.SemaphoreType.DMA((ways,)),
            pltpu.SemaphoreType.DMA((ways,)),
            pltpu.SemaphoreType.DMA,
            pltpu.SemaphoreType.DMA,
        ],
        compiler_params=pltpu.CompilerParams(collective_id=0, has_side_effects=True),
    )(
        neighbour_lists.reshape(cells, 1, width),
        jnp.transpose(halo_counts, (1, 2, 0)),
        positions_now.reshape(cells, 4, slots),
        rows(positions_next),
        rows(velocities),
        descendants.reshape(cells, 2, slots),
    )
    return (drift.reshape(cx, cy, cz, 3, slots), tension.reshape(cx, cy, cz, slots))


def solution(mesh):
    return jax.shard_map(
        shards,
        mesh=mesh,
        in_specs=(
            P("gx", "gy", "gz", None, None),
            P("gx", "gy", "gz", None, None),
            P("gx", "gy", "gz", None, None),
            P("gx", "gy", "gz"),
            P("gx", "gy", "gz", None),
            P("gx", "gy", "gz", None, None),
        ),
        out_specs=(P("gx", "gy", "gz", None, None), P("gx", "gy", "gz", None)),
        check_vma=False,
    )
```

```python
import functools

import jax
import jax.numpy as jnp
from jax import lax
from jax.experimental import pallas as pl
from jax.experimental.pallas import tpu as pltpu
from jax.sharding import PartitionSpec as P

EPS_SQ = 0.01
STEP_DT = 0.3
HALF_KICK = 0.045
AXES = ("gx", "gy", "gz")
GROUP = 8
ROWS = 32
MESH = pl.DeviceIdType.MESH


def pieces(tile):
    first = tile.astype(jnp.bfloat16).astype(jnp.float32)
    rest = tile - first
    second = rest.astype(jnp.bfloat16).astype(jnp.float32)
    return first, second, rest - second


def kernel(
    dims, width, sizes, lists, counts, pos_hbm, next_hbm, vel_hbm, desc_hbm, drift_ref, tension_ref,
    pos, nxt, vel, desc, now_pad, next_pad, feats, moms, lhs, squared, stat, inbox,
    load_sems, now_send, now_recv, next_send, next_recv, stat_send, stat_recv,
):
    cx, cy, cz = dims
    sx, sy, sz = sizes
    py, pz = cy + 2, cz + 2
    cells = cx * cy * cz
    slots = pos.shape[-1]
    folded = sz == 2 and cz == 1
    total = sx * sy * sz
    me = tuple(lax.axis_index(name) for name in AXES)
    row8 = lax.broadcasted_iota(jnp.int32, (8, slots), 0)
    row4 = lax.broadcasted_iota(jnp.int32, (4, slots), 0)
    lane4 = lax.broadcasted_iota(jnp.int32, (4, slots), 1)

    loads = [
        pltpu.make_async_copy(src, dst, load_sems.at[i])
        for i, (src, dst) in enumerate(((pos_hbm, pos), (next_hbm, nxt), (vel_hbm, vel), (desc_hbm, desc)))
    ]
    for load in loads:
        load.start()

    def peer(step):
        where = []
        at = step
        for mine, size in zip(reversed(me), reversed(sizes)):
            where.append(lax.rem(mine + at % size, size))
            at = at // size
        return tuple(reversed(where))

    def each_peer(act):
        if total <= 64:
            for step in range(1, total):
                act(step, peer(step))
        else:
            lax.fori_loop(1, total, lambda step, _: (act(step, peer(step)), 0)[1], 0)

    barrier = pltpu.get_barrier_semaphore()
    each_peer(lambda step, who: pl.semaphore_signal(barrier, inc=1, device_id=who, device_id_type=MESH))

    def plane(iz, dz):
        return (1 if dz == 0 else 0) if folded else iz + 1 + dz

    def split(n):
        return n // (cy * cz), n // cz % cy, n % cz

    def shift_of(ix, iy, iz):
        fx = ix.astype(jnp.float32) - (cx + 2) / 2
        fy = iy.astype(jnp.float32) - (cy + 2) / 2
        fz = iz.astype(jnp.float32) - (cz + 2) / 2
        return jnp.where(row4 == 0, fx, jnp.where(row4 == 1, fy, jnp.where(row4 == 2, fz, 0.0)))

    loads[0].wait()
    loads[1].wait()

    def stage(n, _):
        ix, iy, iz = split(n)
        tile = pos[n]
        now_pad[ix + 1, iy + 1, plane(iz, 0)] = jnp.where((row4 == 3) & (lane4 >= counts[iy, iz, ix]), 0.0, tile)
        rows = [nxt[pl.ds(3 * n + r, 1), :] for r in range(3)]
        next_pad[ix + 1, iy + 1, plane(iz, 0)] = jnp.concatenate(rows + [jnp.zeros_like(rows[0])], axis=0)
        return 0

    lax.fori_loop(0, cells, stage, 0, unroll=4)

    def face(d, size):
        if d == 0:
            return pl.ds(1, size), pl.ds(1, size)
        return (pl.ds(size, 1), pl.ds(0, 1)) if d > 0 else (pl.ds(1, 1), pl.ds(size + 1, 1))

    ways = [
        (dx, dy, dz)
        for dz in ((0, 1) if folded else (0, 1, -1))
        for dx in (0, 1, -1)
        for dy in (0, 1, -1)
        if (dx, dy, dz) != (0, 0, 0)
    ]
    ways.sort(key=lambda way: (way[2] == 0, abs(way[0]) + abs(way[1])))

    def exchange(buf, send_sems, recv_sems):
        made = []
        for i, (dx, dy, dz) in enumerate(ways):
            fx, tx = face(dx, cx)
            fy, ty = face(dy, cy)
            if folded:
                fz, tz = pl.ds(1, 1), pl.ds(1 - dz, 1)
            else:
                fz, tz = face(dz, cz)
            who = tuple(lax.rem(mine + d + size, size) for mine, d, size in zip(me, (dx, dy, dz), sizes))
            made.append(
                pltpu.make_async_remote_copy(
                    src_ref=buf.at[fx, fy, fz],
                    dst_ref=buf.at[tx, ty, tz],
                    send_sem=send_sems.at[i],
                    recv_sem=recv_sems.at[i],
                    device_id=who,
                    device_id_type=MESH,
                )
            )
        for copy in made:
            copy.start()
        return made

    pl.semaphore_wait(barrier, total - 1)
    now_copies = exchange(now_pad, now_send, now_recv)
    next_copies = exchange(next_pad, next_send, next_recv)

    units = jnp.where(row8 < 3, 1.0, 0.0)

    def prepare(px, py_, image, at_plane):
        tile = now_pad[px, py_, at_plane]
        spot = tile + shift_of(jnp.int32(px), jnp.int32(py_), jnp.int32(image))
        square = spot * spot
        size = square[0:1] + square[1:2] + square[2:3]
        base = jnp.where(row4 == 3, size, spot)
        a, b, c = pieces(jnp.concatenate([base, base], axis=0))
        index = (px * py + py_) * pz + image
        rows = jnp.concatenate([a, jnp.where(row8 < 4, a, b), jnp.where(row8 < 4, b, c), units], axis=0)
        feats[index, :, 0:ROWS] = rows.astype(jnp.bfloat16).T
        mass = tile[3:4]
        mom = jnp.where(row4 == 3, mass, spot * mass)
        mom = jnp.concatenate([mom, jnp.zeros_like(mom)], axis=0)
        high = mom.astype(jnp.bfloat16).astype(jnp.float32)
        moms[index] = jnp.concatenate([high, mom - high], axis=0).astype(jnp.bfloat16)
        return spot, size

    def mine(n, _):
        ix, iy, iz = split(n)
        spot, size = prepare(ix + 1, iy + 1, iz + 1, plane(iz, 0))
        base = jnp.where(row4 == 3, 1.0, -2.0 * spot)
        a, b, c = pieces(jnp.concatenate([base, base], axis=0))
        n1, n2, n3 = pieces(jnp.broadcast_to(size + EPS_SQ, (8, slots)))
        norm = jnp.where(row8 == 0, n1, jnp.where(row8 == 1, n2, jnp.where(row8 == 2, n3, 0.0)))
        rows = jnp.concatenate([jnp.where(row8 < 4, a, b), jnp.where(row8 < 4, c, a), jnp.where(row8 < 4, b, a), norm], axis=0)
        lhs[n] = rows.astype(jnp.bfloat16)
        return 0

    def clear(i, _):
        feats[i] = jnp.zeros((slots, slots), jnp.bfloat16)
        return 0

    lax.fori_loop(0, feats.shape[0], clear, 0, unroll=6)
    lax.fori_loop(0, cells, mine, 0, unroll=4)
    for copy in now_copies:
        copy.wait()

    def rim_x(i, _):
        for px in (0, cx + 1):
            prepare(px, i // cz, i % cz + 1, plane(i % cz, 0))
        return 0

    def rim_y(i, _):
        for py_ in (0, cy + 1):
            prepare(i // cz + 1, py_, i % cz + 1, plane(i % cz, 0))
        return 0

    def rim_z(i, _):
        for image, dz in ((0, -1), (cz + 1, 1)):
            prepare(i // py, i % py, image, plane(0 if dz < 0 else cz - 1, dz))
        return 0

    lax.fori_loop(0, py * cz, rim_x, 0, unroll=2)
    lax.fori_loop(0, cx * cz, rim_y, 0, unroll=2)
    lax.fori_loop(0, (cx + 2) * py, rim_z, 0, unroll=2)
    for copy in next_copies:
        copy.wait()
    loads[2].wait()
    loads[3].wait()

    def pull(n):
        ix, iy, iz = split(n)
        corner = (ix * py + iy) * pz + iz
        own = lhs[n]
        blank = jnp.zeros((slots - ROWS, slots), jnp.bfloat16)
        own = jnp.concatenate([own, blank], axis=0)
        none = jnp.zeros_like(own)
        both = jnp.concatenate(
            [jnp.concatenate([own, none], axis=1), jnp.concatenate([none, own], axis=1)], axis=0
        )
        sources = []
        for k in range(width):
            code = lists[n, 0, k]
            d9 = (code * 57) >> 9
            d3 = (code * 43) >> 7
            sources.append(corner + d9 * (py * pz) + (d3 - 3 * d9) * pz + code - 3 * d3)
        acc = jnp.zeros((16, 2 * slots), jnp.float32)
        for k in range(0, width, 2):
            pair = sources[k : k + 2]
            x = jnp.concatenate([feats[s] for s in pair], axis=1)
            z = jnp.concatenate([moms[s] for s in pair], axis=1)
            inv = lax.rsqrt(jnp.dot(x, both, preferred_element_type=jnp.float32))
            weight = inv * inv * inv
            high = weight.astype(jnp.bfloat16)
            low = (weight - high.astype(jnp.float32)).astype(jnp.bfloat16)
            w = jnp.concatenate(
                [jnp.concatenate([high[:, h * slots : (h + 1) * slots], low[:, h * slots : (h + 1) * slots]], axis=1) for h in range(2)], axis=0
            )
            acc += jnp.dot(z, w, preferred_element_type=jnp.float32)
        acc = acc[:, :slots] + acc[:, slots:]
        return acc[0:4] + acc[8:12]

    def target(n, stats):
        ix, iy, iz = split(n)
        sums = pull(n)
        tile = now_pad[ix + 1, iy + 1, plane(iz, 0)]
        accel = sums - (tile + shift_of(ix + 1, iy + 1, iz + 1)) * sums[3:4]
        rows = [vel[pl.ds(3 * n + r, 1), :] for r in range(3)]
        speed = jnp.concatenate(rows + [jnp.zeros_like(rows[0])], axis=0)
        predicted = tile + STEP_DT * speed + HALF_KICK * accel
        links = desc[n]
        dcode = links[0:1]
        d9 = (dcode * 57) >> 9
        d3 = (dcode * 43) >> 7
        dz = dcode - 3 * d3
        d3 = jnp.broadcast_to(d3, (8, slots))
        dslot = jnp.broadcast_to(links[1:2], (8, slots))
        found = [jnp.zeros((8, slots), jnp.float32)] * (1 if folded else 2)
        for c in range(9):
            at = (ix + c // 3, iy + c % 3)
            tiles = [next_pad[at + (plane(iz, d),)] for d in ((-1, 0) if folded else (-1, 0, 1))]
            if not folded:
                tiles.append(jnp.zeros_like(tiles[0]))
            for h in range(len(tiles) // 2):
                got = jnp.take_along_axis(jnp.concatenate(tiles[2 * h : 2 * h + 2], axis=0), dslot, axis=1)
                found[h] = jnp.where(d3 == c, got, found[h])
        if folded:
            there = jnp.where(dz == 1, found[0][4:8], found[0][0:4])
        else:
            there = jnp.where(dz == 1, found[0][4:8], jnp.where(dz == 0, found[0][0:4], found[1][0:4]))
        step = jnp.where(row4 == 0, d9, jnp.where(row4 == 1, d3[0:4] - 3 * d9, dz)).astype(jnp.float32) - 1.0
        live = lane4 < counts[iy, iz, ix]
        error = jnp.where(live & (row4 < 3), step + there - predicted, 0.0)
        for r in range(3):
            drift_ref[pl.ds(3 * n + r, 1), :] = error[r : r + 1]
        summed = jnp.sum(error * error, axis=0, keepdims=True)
        squared[pl.ds(n, 1), :] = summed
        return stats + jnp.where(row8 == 0, summed, jnp.where((row8 == 1) & live[0:1], 1.0, 0.0))

    group = GROUP if cells % GROUP == 0 else 1

    def several(i, stats):
        for u in range(group):
            stats = target(i * group + u, stats)
        return stats

    stats = lax.fori_loop(0, cells // group, several, jnp.zeros((8, slots), jnp.float32))
    stat[...] = stats[0:2]

    def report(step, who):
        pltpu.make_async_remote_copy(
            src_ref=stat,
            dst_ref=inbox.at[step - 1],
            send_sem=stat_send,
            recv_sem=stat_recv,
            device_id=who,
            device_id_type=MESH,
        ).start()

    each_peer(report)
    pltpu.make_async_copy(inbox, inbox, stat_recv).wait()
    sums = stat[...] + jnp.sum(inbox[...], axis=0)
    mean_sq = jnp.sum(sums[0:1], axis=1, keepdims=True) / jnp.sum(sums[1:2], axis=1, keepdims=True)
    tension_ref[...] = squared[...] / (mean_sq + 1e-06)
    pltpu.make_async_copy(inbox, inbox, stat_send).wait()


def shards(positions_now, velocities, positions_next, halo_counts, neighbour_lists, descendants):
    slots = positions_now.shape[-1]
    cx, cy, cz, width = neighbour_lists.shape
    cells = cx * cy * cz
    sizes = tuple(lax.axis_size(name) for name in AXES)
    folded = sizes[2] == 2 and cz == 1
    planes = 2 if folded else cz + 2
    padded = (cx + 2) * (cy + 2) * (cz + 2)
    ways = 17 if folded else 26
    peers = sizes[0] * sizes[1] * sizes[2] - 1

    def rows(array):
        return jnp.transpose(array, (0, 1, 2, 3, 4)).reshape(cells * 3, slots)

    drift, tension = pl.pallas_call(
        functools.partial(kernel, (cx, cy, cz), width, sizes),
        out_shape=(
            jax.ShapeDtypeStruct((cells * 3, slots), jnp.float32),
            jax.ShapeDtypeStruct((cells, slots), jnp.float32),
        ),
        in_specs=[pl.BlockSpec(memory_space=pltpu.SMEM)] * 2 + [pl.BlockSpec(memory_space=pl.ANY)] * 4,
        out_specs=(pl.BlockSpec(memory_space=pltpu.VMEM),) * 2,
        scratch_shapes=[
            pltpu.VMEM((cells, 4, slots), jnp.float32),
            pltpu.VMEM((cells * 3, slots), jnp.float32),
            pltpu.VMEM((cells * 3, slots), jnp.float32),
            pltpu.VMEM((cells, 2, slots), jnp.int32),
            pltpu.VMEM((cx + 2, cy + 2, planes, 4, slots), jnp.float32),
            pltpu.VMEM((cx + 2, cy + 2, planes, 4, slots), jnp.float32),
            pltpu.VMEM((padded, slots, slots), jnp.bfloat16),
            pltpu.VMEM((padded, 16, slots), jnp.bfloat16),
            pltpu.VMEM((cells, ROWS, slots), jnp.bfloat16),
            pltpu.VMEM((cells, slots), jnp.float32),
            pltpu.VMEM((2, slots), jnp.float32),
            pltpu.VMEM((peers, 2, slots), jnp.float32),
            pltpu.SemaphoreType.DMA((4,)),
            pltpu.SemaphoreType.DMA((ways,)),
            pltpu.SemaphoreType.DMA((ways,)),
            pltpu.SemaphoreType.DMA((ways,)),
            pltpu.SemaphoreType.DMA((ways,)),
            pltpu.SemaphoreType.DMA,
            pltpu.SemaphoreType.DMA,
        ],
        compiler_params=pltpu.CompilerParams(collective_id=0, has_side_effects=True),
    )(
        neighbour_lists.reshape(cells, 1, width),
        jnp.transpose(halo_counts, (1, 2, 0)),
        positions_now.reshape(cells, 4, slots),
        rows(positions_next),
        rows(velocities),
        descendants.reshape(cells, 2, slots),
    )
    return (drift.reshape(cx, cy, cz, 3, slots), tension.reshape(cx, cy, cz, slots))


def solution(mesh):
    return jax.shard_map(
        shards,
        mesh=mesh,
        in_specs=(
            P("gx", "gy", "gz", None, None),
            P("gx", "gy", "gz", None, None),
            P("gx", "gy", "gz", None, None),
            P("gx", "gy", "gz"),
            P("gx", "gy", "gz", None),
            P("gx", "gy", "gz", None, None),
        ),
        out_specs=(P("gx", "gy", "gz", None, None), P("gx", "gy", "gz", None)),
        check_vma=False,
    )
```

```python
import functools

import jax
import jax.numpy as jnp
from jax import lax
from jax.experimental import pallas as pl
from jax.experimental.pallas import tpu as pltpu
from jax.sharding import PartitionSpec as P

EPS_SQ = 0.01
STEP_DT = 0.3
HALF_KICK = 0.045
AXES = ("gx", "gy", "gz")
GROUP = 16
ROWS = 32
MESH = pl.DeviceIdType.MESH


def pieces(tile):
    first = tile.astype(jnp.bfloat16).astype(jnp.float32)
    rest = tile - first
    second = rest.astype(jnp.bfloat16).astype(jnp.float32)
    return first, second, rest - second


def kernel(
    dims, width, sizes, lists_hbm, counts_hbm, pos_hbm, next_hbm, vel_hbm, desc_hbm, ends_hbm, tension_hbm,
    lists, counts, pos, nxt, vel, desc, now_pad, next_pad, feats, moms, lhs, ends, squared, tension, stat, inbox,
    load_sems, end_sem, now_send, now_recv, next_send, next_recv, stat_send, stat_recv,
):
    cx, cy, cz = dims
    sx, sy, sz = sizes
    py, pz = cy + 2, cz + 2
    cells = cx * cy * cz
    slots = pos.shape[-1]
    folded = sz == 2 and cz == 1
    total = sx * sy * sz
    me = tuple(lax.axis_index(name) for name in AXES)
    row8 = lax.broadcasted_iota(jnp.int32, (8, slots), 0)
    row4 = lax.broadcasted_iota(jnp.int32, (4, slots), 0)
    lane4 = lax.broadcasted_iota(jnp.int32, (4, slots), 1)

    loads = [
        pltpu.make_async_copy(src, dst, load_sems.at[i])
        for i, (src, dst) in enumerate(
            ((counts_hbm, counts), (pos_hbm, pos), (next_hbm, nxt), (lists_hbm, lists), (vel_hbm, vel), (desc_hbm, desc))
        )
    ]
    for load in loads:
        load.start()

    def peer(step):
        where = []
        at = step
        for mine, size in zip(reversed(me), reversed(sizes)):
            where.append(lax.rem(mine + at % size, size))
            at = at // size
        return tuple(reversed(where))

    def far(step):
        gaps = (step // (sy * sz), step // sz % sy, step % sz)
        near = [min(gap, size - gap) for gap, size in zip(gaps, sizes)]
        return max(near) > 1, sum(near)

    def each_peer(act, outward=True):
        if total <= 64:
            for step in sorted(range(1, total), key=far, reverse=not outward):
                act(step, peer(step))
        else:
            lax.fori_loop(1, total, lambda step, _: (act(step, peer(step)), 0)[1], 0)

    barrier = pltpu.get_barrier_semaphore()
    each_peer(lambda step, who: pl.semaphore_signal(barrier, inc=1, device_id=who, device_id_type=MESH))

    def plane(iz, dz):
        return (1 if dz == 0 else 0) if folded else iz + 1 + dz

    def split(n):
        return n // (cy * cz), n // cz % cy, n % cz

    def shift_of(ix, iy, iz):
        fx = ix.astype(jnp.float32) - (cx + 2) / 2
        fy = iy.astype(jnp.float32) - (cy + 2) / 2
        fz = iz.astype(jnp.float32) - (cz + 2) / 2
        return jnp.where(row4 == 0, fx, jnp.where(row4 == 1, fy, jnp.where(row4 == 2, fz, 0.0)))

    def stage_now(n, _):
        ix, iy, iz = split(n)
        now_pad[ix + 1, iy + 1, plane(iz, 0)] = jnp.where((row4 == 3) & (lane4 >= counts[iy, iz, ix]), 0.0, pos[n])
        return 0

    def stage_next(n, _):
        ix, iy, iz = split(n)
        rows = [nxt[pl.ds(3 * n + r, 1), :] for r in range(3)]
        next_pad[ix + 1, iy + 1, plane(iz, 0)] = jnp.concatenate(rows + [jnp.zeros_like(rows[0])], axis=0)
        return 0

    def face(d, size):
        if d == 0:
            return pl.ds(1, size), pl.ds(1, size)
        return (pl.ds(size, 1), pl.ds(0, 1)) if d > 0 else (pl.ds(1, 1), pl.ds(size + 1, 1))

    ways = [
        (dx, dy, dz)
        for dz in ((0, 1) if folded else (0, 1, -1))
        for dx in (0, 1, -1)
        for dy in (0, 1, -1)
        if (dx, dy, dz) != (0, 0, 0)
    ]
    ways.sort(key=lambda way: ((way[0], way[1]) != (0, 0), way[2] != 0, abs(way[0]) + abs(way[1])))

    def exchange(buf, send_sems, recv_sems):
        made = []
        for i, (dx, dy, dz) in enumerate(ways):
            fx, tx = face(dx, cx)
            fy, ty = face(dy, cy)
            if folded:
                fz, tz = pl.ds(1, 1), pl.ds(1 - dz, 1)
            else:
                fz, tz = face(dz, cz)
            who = tuple(lax.rem(mine + d + size, size) for mine, d, size in zip(me, (dx, dy, dz), sizes))
            made.append(
                pltpu.make_async_remote_copy(
                    src_ref=buf.at[fx, fy, fz],
                    dst_ref=buf.at[tx, ty, tz],
                    send_sem=send_sems.at[i],
                    recv_sem=recv_sems.at[i],
                    device_id=who,
                    device_id_type=MESH,
                )
            )
        for copy in made:
            copy.start()
        return made

    loads[0].wait()
    loads[1].wait()
    lax.fori_loop(0, cells, stage_now, 0, unroll=8)
    pl.semaphore_wait(barrier, total - 1)
    now_copies = exchange(now_pad, now_send, now_recv)
    loads[2].wait()
    lax.fori_loop(0, cells, stage_next, 0, unroll=8)
    next_copies = exchange(next_pad, next_send, next_recv)

    units = jnp.where(row8 < 3, 1.0, 0.0)

    def prepare(px, py_, image, at_plane):
        tile = now_pad[px, py_, at_plane]
        spot = tile + shift_of(jnp.int32(px), jnp.int32(py_), jnp.int32(image))
        square = spot * spot
        size = square[0:1] + square[1:2] + square[2:3]
        base = jnp.where(row4 == 3, size, spot)
        a, b, c = pieces(jnp.concatenate([base, base], axis=0))
        index = (px * py + py_) * pz + image
        rows = jnp.concatenate([a, jnp.where(row8 < 4, a, b), jnp.where(row8 < 4, b, c), units], axis=0)
        rows = rows.astype(jnp.bfloat16)
        feats[index, :, 0 : 2 * ROWS] = jnp.concatenate([rows, rows], axis=0).T
        mass = tile[3:4]
        mom = jnp.where(row4 == 3, mass, spot * mass)
        mom = jnp.concatenate([mom, jnp.zeros_like(mom)], axis=0)
        high = mom.astype(jnp.bfloat16).astype(jnp.float32)
        moms[index] = jnp.concatenate([high, mom - high], axis=0).astype(jnp.bfloat16)
        return spot, size

    def mine(n, _):
        ix, iy, iz = split(n)
        spot, size = prepare(ix + 1, iy + 1, iz + 1, plane(iz, 0))
        base = jnp.where(row4 == 3, 1.0, -2.0 * spot)
        a, b, c = pieces(jnp.concatenate([base, base], axis=0))
        n1, n2, n3 = pieces(jnp.broadcast_to(size + EPS_SQ, (8, slots)))
        norm = jnp.where(row8 == 0, n1, jnp.where(row8 == 1, n2, jnp.where(row8 == 2, n3, 0.0)))
        rows = jnp.concatenate([jnp.where(row8 < 4, a, b), jnp.where(row8 < 4, c, a), jnp.where(row8 < 4, b, a), norm], axis=0)
        lhs[n] = rows.astype(jnp.bfloat16)
        return 0

    lax.fori_loop(0, cells, mine, 0, unroll=8)

    def settle(pick):
        for way, copy in zip(ways, now_copies):
            if pick(*way):
                copy.wait()

    def over(length, body):
        lax.fori_loop(0, length, lambda i, _: (body(i), 0)[1], 0, unroll=True if length <= 8 else 4)

    def both_images(px, py_):
        for image, iz, dz in ((0, 0, -1), (cz + 1, cz - 1, 1)):
            prepare(px, py_, image, plane(iz, dz))

    def rim_x(i):
        for px in (0, cx + 1):
            prepare(px, i // cz, i % cz + 1, plane(i % cz, 0))

    def rim_y(i):
        for py_ in (0, cy + 1):
            prepare(i // cz + 1, py_, i % cz + 1, plane(i % cz, 0))

    settle(lambda dx, dy, dz: dz == 0)
    over(py * cz, rim_x)
    over(cx * cz, rim_y)
    settle(lambda dx, dy, dz: dz != 0 and dx == 0 and dy == 0)
    over(cx * cy, lambda i: both_images(i // cy + 1, i % cy + 1))
    settle(lambda dx, dy, dz: dz != 0 and (dx != 0 or dy != 0))
    over(py, lambda i: [both_images(px, i) for px in (0, cx + 1)])
    over(cx, lambda i: [both_images(i + 1, py_) for py_ in (0, cy + 1)])
    for copy in next_copies:
        copy.wait()
    for load in loads[3:]:
        load.wait()

    first_half = lax.broadcasted_iota(jnp.int32, (slots, 2 * ROWS), 1) < ROWS

    def pull(n):
        ix, iy, iz = split(n)
        corner = (ix * py + iy) * pz + iz
        own = lhs[n]
        none = jnp.zeros_like(own)
        both = jnp.concatenate(
            [jnp.concatenate([own, none], axis=1), jnp.concatenate([none, own], axis=1)], axis=0
        )
        sources = []
        for k in range(width):
            code = lists[n, 0, k]
            d9 = (code * 57) >> 9
            d3 = (code * 43) >> 7
            sources.append(corner + d9 * (py * pz) + (d3 - 3 * d9) * pz + code - 3 * d3)
        acc = jnp.zeros((16, 2 * slots), jnp.float32)
        for k in range(0, width, 2):
            pair = sources[k : k + 2]
            x = jnp.where(first_half, feats[pair[0], :, 0 : 2 * ROWS], feats[pair[-1], :, 0 : 2 * ROWS])
            z = jnp.concatenate([moms[s] for s in pair], axis=1)
            inv = lax.rsqrt(jnp.dot(x, both, preferred_element_type=jnp.float32))
            weight = inv * inv * inv
            high = weight.astype(jnp.bfloat16)
            low = (weight - high.astype(jnp.float32)).astype(jnp.bfloat16)
            w = jnp.concatenate(
                [jnp.concatenate([high[:, h * slots : (h + 1) * slots], low[:, h * slots : (h + 1) * slots]], axis=1) for h in range(2)], axis=0
            )
            acc += jnp.dot(z, w, preferred_element_type=jnp.float32)
        acc = acc[:, :slots] + acc[:, slots:]
        return acc[0:4] + acc[8:12]

    def target(n, stats):
        ix, iy, iz = split(n)
        sums = pull(n)
        tile = now_pad[ix + 1, iy + 1, plane(iz, 0)]
        accel = sums - (tile + shift_of(ix + 1, iy + 1, iz + 1)) * sums[3:4]
        rows = [vel[pl.ds(3 * n + r, 1), :] for r in range(3)]
        speed = jnp.concatenate(rows + [jnp.zeros_like(rows[0])], axis=0)
        predicted = tile + STEP_DT * speed + HALF_KICK * accel
        links = desc[n]
        dcode = links[0:1]
        d9 = (dcode * 57) >> 9
        d3 = (dcode * 43) >> 7
        dz = dcode - 3 * d3
        d3 = jnp.broadcast_to(d3, (8, slots))
        dslot = jnp.broadcast_to(links[1:2], (8, slots))
        found = [jnp.zeros((8, slots), jnp.float32)] * (1 if folded else 2)
        for c in range(9):
            at = (ix + c // 3, iy + c % 3)
            tiles = [next_pad[at + (plane(iz, d),)] for d in ((-1, 0) if folded else (-1, 0, 1))]
            if not folded:
                tiles.append(jnp.zeros_like(tiles[0]))
            for h in range(len(tiles) // 2):
                got = jnp.take_along_axis(jnp.concatenate(tiles[2 * h : 2 * h + 2], axis=0), dslot, axis=1)
                found[h] = jnp.where(d3 == c, got, found[h])
        if folded:
            there = jnp.where(dz == 1, found[0][4:8], found[0][0:4])
        else:
            there = jnp.where(dz == 1, found[0][4:8], jnp.where(dz == 0, found[0][0:4], found[1][0:4]))
        step = jnp.where(row4 == 0, d9, jnp.where(row4 == 1, d3[0:4] - 3 * d9, dz)).astype(jnp.float32) - 1.0
        live = lane4 < counts[iy, iz, ix]
        error = jnp.where(live & (row4 < 3), step + there - predicted, 0.0)
        for r in range(3):
            ends[pl.ds(3 * n + r, 1), :] = error[r : r + 1]
        summed = jnp.sum(error * error, axis=0, keepdims=True)
        squared[pl.ds(n, 1), :] = summed
        return stats + jnp.where(row8 == 0, summed, jnp.where((row8 == 1) & live[0:1], 1.0, 0.0))

    group = GROUP if cells % GROUP == 0 else 1

    def several(i, stats):
        for u in range(group):
            stats = target(i * group + u, stats)
        return stats

    stats = lax.fori_loop(0, cells // group, several, jnp.zeros((8, slots), jnp.float32))
    stat[...] = stats[0:2]
    keep = pltpu.make_async_copy(ends, ends_hbm, end_sem.at[0])
    keep.start()

    def report(step, who):
        pltpu.make_async_remote_copy(
            src_ref=stat,
            dst_ref=inbox.at[step - 1],
            send_sem=stat_send,
            recv_sem=stat_recv,
            device_id=who,
            device_id_type=MESH,
        ).start()

    each_peer(report, outward=False)
    pltpu.make_async_copy(inbox, inbox, stat_recv).wait()
    sums = stat[...] + jnp.sum(inbox[...], axis=0)
    mean_sq = jnp.sum(sums[0:1], axis=1, keepdims=True) / jnp.sum(sums[1:2], axis=1, keepdims=True)
    tension[...] = squared[...] / (mean_sq + 1e-06)
    last = pltpu.make_async_copy(tension, tension_hbm, end_sem.at[1])
    last.start()
    pltpu.make_async_copy(inbox, inbox, stat_send).wait()
    keep.wait()
    last.wait()


def shards(positions_now, velocities, positions_next, halo_counts, neighbour_lists, descendants):
    slots = positions_now.shape[-1]
    cx, cy, cz, width = neighbour_lists.shape
    cells = cx * cy * cz
    sizes = tuple(lax.axis_size(name) for name in AXES)
    folded = sizes[2] == 2 and cz == 1
    planes = 2 if folded else cz + 2
    padded = (cx + 2) * (cy + 2) * (cz + 2)
    ways = 17 if folded else 26
    peers = sizes[0] * sizes[1] * sizes[2] - 1

    def rows(array):
        return jnp.transpose(array, (0, 1, 2, 3, 4)).reshape(cells * 3, slots)

    ends, tension = pl.pallas_call(
        functools.partial(kernel, (cx, cy, cz), width, sizes),
        out_shape=(
            jax.ShapeDtypeStruct((cells * 3, slots), jnp.float32),
            jax.ShapeDtypeStruct((cells, slots), jnp.float32),
        ),
        in_specs=[pl.BlockSpec(memory_space=pl.ANY)] * 6,
        out_specs=(pl.BlockSpec(memory_space=pl.ANY),) * 2,
        scratch_shapes=[
            pltpu.SMEM((cells, 1, width), jnp.int32),
            pltpu.SMEM((cy, cz, cx), jnp.int32),
            pltpu.VMEM((cells, 4, slots), jnp.float32),
            pltpu.VMEM((cells * 3, slots), jnp.float32),
            pltpu.VMEM((cells * 3, slots), jnp.float32),
            pltpu.VMEM((cells, 2, slots), jnp.int32),
            pltpu.VMEM((cx + 2, cy + 2, planes, 4, slots), jnp.float32),
            pltpu.VMEM((cx + 2, cy + 2, planes, 4, slots), jnp.float32),
            pltpu.VMEM((padded, slots, slots), jnp.bfloat16),
            pltpu.VMEM((padded, 16, slots), jnp.bfloat16),
            pltpu.VMEM((cells, ROWS, slots), jnp.bfloat16),
            pltpu.VMEM((cells * 3, slots), jnp.float32),
            pltpu.VMEM((cells, slots), jnp.float32),
            pltpu.VMEM((cells, slots), jnp.float32),
            pltpu.VMEM((2, slots), jnp.float32),
            pltpu.VMEM((peers, 2, slots), jnp.float32),
            pltpu.SemaphoreType.DMA((6,)),
            pltpu.SemaphoreType.DMA((2,)),
            pltpu.SemaphoreType.DMA((ways,)),
            pltpu.SemaphoreType.DMA((ways,)),
            pltpu.SemaphoreType.DMA((ways,)),
            pltpu.SemaphoreType.DMA((ways,)),
            pltpu.SemaphoreType.DMA,
            pltpu.SemaphoreType.DMA,
        ],
        compiler_params=pltpu.CompilerParams(collective_id=0, has_side_effects=True),
    )(
        neighbour_lists.reshape(cells, 1, width),
        jnp.transpose(halo_counts, (1, 2, 0)),
        positions_now.reshape(cells, 4, slots),
        rows(positions_next),
        rows(velocities),
        descendants.reshape(cells, 2, slots),
    )
    drift = ends
    return (drift.reshape(cx, cy, cz, 3, slots), tension.reshape(cx, cy, cz, slots))


def solution(mesh):
    return jax.shard_map(
        shards,
        mesh=mesh,
        in_specs=(
            P("gx", "gy", "gz", None, None),
            P("gx", "gy", "gz", None, None),
            P("gx", "gy", "gz", None, None),
            P("gx", "gy", "gz"),
            P("gx", "gy", "gz", None),
            P("gx", "gy", "gz", None, None),
        ),
        out_specs=(P("gx", "gy", "gz", None, None), P("gx", "gy", "gz", None)),
        check_vma=False,
    )
```

```python
import functools

import jax
import jax.numpy as jnp
from jax import lax
from jax.experimental import pallas as pl
from jax.experimental.pallas import tpu as pltpu
from jax.sharding import PartitionSpec as P

EPS_SQ = 0.01
STEP_DT = 0.3
HALF_KICK = 0.045
AXES = ("gx", "gy", "gz")
GROUP = 16
ROWS = 32
MESH = pl.DeviceIdType.MESH


def pieces(tile):
    first = tile.astype(jnp.bfloat16).astype(jnp.float32)
    rest = tile - first
    second = rest.astype(jnp.bfloat16).astype(jnp.float32)
    return first, second, rest - second


def kernel(
    dims, width, sizes, lists_hbm, counts_hbm, pos_hbm, next_hbm, vel_hbm, desc_hbm, ends_hbm, tension_hbm,
    lists, counts, pos, nxt, vel, desc, now_pad, next_pad, feats, moms, lhs, ends, squared, tension, stat, inbox,
    load_sems, end_sem, now_send, now_recv, next_send, next_recv, stat_send, stat_recv,
):
    cx, cy, cz = dims
    sx, sy, sz = sizes
    py, pz = cy + 2, cz + 2
    cells = cx * cy * cz
    slots = pos.shape[-1]
    folded = sz == 2 and cz == 1
    total = sx * sy * sz
    me = tuple(lax.axis_index(name) for name in AXES)
    row8 = lax.broadcasted_iota(jnp.int32, (8, slots), 0)
    row4 = lax.broadcasted_iota(jnp.int32, (4, slots), 0)
    lane4 = lax.broadcasted_iota(jnp.int32, (4, slots), 1)

    loads = [
        pltpu.make_async_copy(src, dst, load_sems.at[i])
        for i, (src, dst) in enumerate(
            ((counts_hbm, counts), (pos_hbm, pos), (next_hbm, nxt), (lists_hbm, lists), (vel_hbm, vel), (desc_hbm, desc))
        )
    ]
    for load in loads:
        load.start()

    def peer(step):
        where = []
        at = step
        for mine, size in zip(reversed(me), reversed(sizes)):
            where.append(lax.rem(mine + at % size, size))
            at = at // size
        return tuple(reversed(where))

    def far(step):
        gaps = (step // (sy * sz), step // sz % sy, step % sz)
        near = [min(gap, size - gap) for gap, size in zip(gaps, sizes)]
        return max(near) > 1, sum(near)

    def each_peer(act, outward=True):
        if total <= 64:
            for step in sorted(range(1, total), key=far, reverse=not outward):
                act(step, peer(step))
        else:
            lax.fori_loop(1, total, lambda step, _: (act(step, peer(step)), 0)[1], 0)

    barrier = pltpu.get_barrier_semaphore()
    each_peer(lambda step, who: pl.semaphore_signal(barrier, inc=1, device_id=who, device_id_type=MESH))

    def plane(iz, dz):
        return (1 if dz == 0 else 0) if folded else iz + 1 + dz

    def split(n):
        return n // (cy * cz), n // cz % cy, n % cz

    def shift_of(ix, iy, iz):
        fx = ix.astype(jnp.float32) - (cx + 2) / 2
        fy = iy.astype(jnp.float32) - (cy + 2) / 2
        fz = iz.astype(jnp.float32) - (cz + 2) / 2
        return jnp.where(row4 == 0, fx, jnp.where(row4 == 1, fy, jnp.where(row4 == 2, fz, 0.0)))

    def stage_now(n, _):
        ix, iy, iz = split(n)
        now_pad[ix + 1, iy + 1, plane(iz, 0)] = jnp.where((row4 == 3) & (lane4 >= counts[iy, iz, ix]), 0.0, pos[n])
        return 0

    def stage_next(n, _):
        ix, iy, iz = split(n)
        rows = [nxt[pl.ds(3 * n + r, 1), :] for r in range(3)]
        next_pad[ix + 1, iy + 1, plane(iz, 0)] = jnp.concatenate(rows + [jnp.zeros_like(rows[0])], axis=0)
        return 0

    def face(d, size):
        if d == 0:
            return pl.ds(1, size), pl.ds(1, size)
        return (pl.ds(size, 1), pl.ds(0, 1)) if d > 0 else (pl.ds(1, 1), pl.ds(size + 1, 1))

    ways = [
        (dx, dy, dz)
        for dz in ((0, 1) if folded else (0, 1, -1))
        for dx in (0, 1, -1)
        for dy in (0, 1, -1)
        if (dx, dy, dz) != (0, 0, 0)
    ]
    ways.sort(key=lambda way: ((way[0], way[1]) != (0, 0), way[2] != 0, abs(way[0]) + abs(way[1])))

    def exchange(buf, send_sems, recv_sems):
        made = []
        for i, (dx, dy, dz) in enumerate(ways):
            fx, tx = face(dx, cx)
            fy, ty = face(dy, cy)
            if folded:
                fz, tz = pl.ds(1, 1), pl.ds(1 - dz, 1)
            else:
                fz, tz = face(dz, cz)
            who = tuple(lax.rem(mine + d + size, size) for mine, d, size in zip(me, (dx, dy, dz), sizes))
            made.append(
                pltpu.make_async_remote_copy(
                    src_ref=buf.at[fx, fy, fz],
                    dst_ref=buf.at[tx, ty, tz],
                    send_sem=send_sems.at[i],
                    recv_sem=recv_sems.at[i],
                    device_id=who,
                    device_id_type=MESH,
                )
            )
        for copy in made:
            copy.start()
        return made

    loads[0].wait()
    loads[1].wait()
    lax.fori_loop(0, cells, stage_now, 0, unroll=8)
    pl.semaphore_wait(barrier, total - 1)
    now_copies = exchange(now_pad, now_send, now_recv)
    loads[2].wait()
    lax.fori_loop(0, cells, stage_next, 0, unroll=8)
    next_copies = exchange(next_pad, next_send, next_recv)

    units = jnp.where(row8 < 3, 1.0, 0.0)

    def prepare(px, py_, image, at_plane):
        tile = now_pad[px, py_, at_plane]
        spot = tile + shift_of(jnp.int32(px), jnp.int32(py_), jnp.int32(image))
        square = spot * spot
        size = square[0:1] + square[1:2] + square[2:3]
        base = jnp.where(row4 == 3, size, spot)
        a, b, c = pieces(jnp.concatenate([base, base], axis=0))
        index = (px * py + py_) * pz + image
        rows = jnp.concatenate([a, jnp.where(row8 < 4, a, b), jnp.where(row8 < 4, b, c), units], axis=0)
        rows = rows.astype(jnp.bfloat16)
        feats[index, :, 0 : 2 * ROWS] = jnp.concatenate([rows, rows], axis=0).T
        mass = tile[3:4]
        mom = jnp.where(row4 == 3, mass, spot * mass)
        mom = jnp.concatenate([mom, jnp.zeros_like(mom)], axis=0)
        high = mom.astype(jnp.bfloat16).astype(jnp.float32)
        moms[index] = jnp.concatenate([high, mom - high], axis=0).astype(jnp.bfloat16)
        return spot, size

    def mine(n, _):
        ix, iy, iz = split(n)
        spot, size = prepare(ix + 1, iy + 1, iz + 1, plane(iz, 0))
        base = jnp.where(row4 == 3, 1.0, -2.0 * spot)
        a, b, c = pieces(jnp.concatenate([base, base], axis=0))
        n1, n2, n3 = pieces(jnp.broadcast_to(size + EPS_SQ, (8, slots)))
        norm = jnp.where(row8 == 0, n1, jnp.where(row8 == 1, n2, jnp.where(row8 == 2, n3, 0.0)))
        rows = jnp.concatenate([jnp.where(row8 < 4, a, b), jnp.where(row8 < 4, c, a), jnp.where(row8 < 4, b, a), norm], axis=0)
        lhs[n] = rows.astype(jnp.bfloat16)
        return 0

    lax.fori_loop(0, cells, mine, 0, unroll=8)

    def settle(pick):
        for way, copy in zip(ways, now_copies):
            if pick(*way):
                copy.wait()

    def over(length, body):
        lax.fori_loop(0, length, lambda i, _: (body(i), 0)[1], 0, unroll=True if length <= 8 else 4)

    def both_images(px, py_):
        for image, iz, dz in ((0, 0, -1), (cz + 1, cz - 1, 1)):
            prepare(px, py_, image, plane(iz, dz))

    def rim_x(i):
        for px in (0, cx + 1):
            prepare(px, i // cz, i % cz + 1, plane(i % cz, 0))

    def rim_y(i):
        for py_ in (0, cy + 1):
            prepare(i // cz + 1, py_, i % cz + 1, plane(i % cz, 0))

    settle(lambda dx, dy, dz: dz == 0)
    over(py * cz, rim_x)
    over(cx * cz, rim_y)
    settle(lambda dx, dy, dz: dz != 0 and dx == 0 and dy == 0)
    over(cx * cy, lambda i: both_images(i // cy + 1, i % cy + 1))
    settle(lambda dx, dy, dz: dz != 0 and (dx != 0 or dy != 0))
    over(py, lambda i: [both_images(px, i) for px in (0, cx + 1)])
    over(cx, lambda i: [both_images(i + 1, py_) for py_ in (0, cy + 1)])
    for copy in next_copies:
        copy.wait()
    for load in loads[3:]:
        load.wait()

    first_half = lax.broadcasted_iota(jnp.int32, (slots, 2 * ROWS), 1) < ROWS

    def pull(n):
        ix, iy, iz = split(n)
        corner = (ix * py + iy) * pz + iz
        own = lhs[n]
        none = jnp.zeros_like(own)
        both = jnp.concatenate(
            [jnp.concatenate([own, none], axis=1), jnp.concatenate([none, own], axis=1)], axis=0
        )
        sources = []
        for k in range(width):
            code = lists[n, 0, k]
            d9 = (code * 57) >> 9
            d3 = (code * 43) >> 7
            sources.append(corner + d9 * (py * pz) + (d3 - 3 * d9) * pz + code - 3 * d3)
        acc = jnp.zeros((16, 2 * slots), jnp.float32)
        for k in range(0, width, 2):
            pair = sources[k : k + 2]
            x = jnp.where(first_half, feats[pair[0], :, 0 : 2 * ROWS], feats[pair[-1], :, 0 : 2 * ROWS])
            z = jnp.concatenate([moms[s] for s in pair], axis=1)
            inv = lax.rsqrt(jnp.dot(x, both, preferred_element_type=jnp.float32))
            weight = inv * inv * inv
            high = weight.astype(jnp.bfloat16)
            low = (weight - high.astype(jnp.float32)).astype(jnp.bfloat16)
            w = jnp.concatenate(
                [jnp.concatenate([high[:, h * slots : (h + 1) * slots], low[:, h * slots : (h + 1) * slots]], axis=1) for h in range(len(pair))], axis=0
            )
            acc += jnp.dot(z, w, preferred_element_type=jnp.float32)
        acc = acc[:, :slots] + acc[:, slots:]
        return acc[0:4] + acc[8:12]

    def target(n, stats):
        ix, iy, iz = split(n)
        sums = pull(n)
        tile = now_pad[ix + 1, iy + 1, plane(iz, 0)]
        accel = sums - (tile + shift_of(ix + 1, iy + 1, iz + 1)) * sums[3:4]
        rows = [vel[pl.ds(3 * n + r, 1), :] for r in range(3)]
        speed = jnp.concatenate(rows + [jnp.zeros_like(rows[0])], axis=0)
        predicted = tile + STEP_DT * speed + HALF_KICK * accel
        links = desc[n]
        dcode = links[0:1]
        d9 = (dcode * 57) >> 9
        d3 = (dcode * 43) >> 7
        dz = dcode - 3 * d3
        d3 = jnp.broadcast_to(d3, (8, slots))
        dslot = jnp.broadcast_to(links[1:2], (8, slots))
        found = [jnp.zeros((8, slots), jnp.float32)] * (1 if folded else 2)
        for c in range(9):
            at = (ix + c // 3, iy + c % 3)
            tiles = [next_pad[at + (plane(iz, d),)] for d in ((-1, 0) if folded else (-1, 0, 1))]
            if not folded:
                tiles.append(jnp.zeros_like(tiles[0]))
            for h in range(len(tiles) // 2):
                got = jnp.take_along_axis(jnp.concatenate(tiles[2 * h : 2 * h + 2], axis=0), dslot, axis=1)
                found[h] = jnp.where(d3 == c, got, found[h])
        if folded:
            there = jnp.where(dz == 1, found[0][4:8], found[0][0:4])
        else:
            there = jnp.where(dz == 1, found[0][4:8], jnp.where(dz == 0, found[0][0:4], found[1][0:4]))
        step = jnp.where(row4 == 0, d9, jnp.where(row4 == 1, d3[0:4] - 3 * d9, dz)).astype(jnp.float32) - 1.0
        live = lane4 < counts[iy, iz, ix]
        error = jnp.where(live & (row4 < 3), step + there - predicted, 0.0)
        for r in range(3):
            ends[pl.ds(3 * n + r, 1), :] = error[r : r + 1]
        summed = jnp.sum(error * error, axis=0, keepdims=True)
        squared[pl.ds(n, 1), :] = summed
        return stats + jnp.where(row8 == 0, summed, jnp.where((row8 == 1) & live[0:1], 1.0, 0.0))

    group = GROUP if cells % GROUP == 0 else 1

    def several(i, stats):
        for u in range(group):
            stats = target(i * group + u, stats)
        return stats

    stats = lax.fori_loop(0, cells // group, several, jnp.zeros((8, slots), jnp.float32))
    stat[...] = stats[0:2]
    keep = pltpu.make_async_copy(ends, ends_hbm, end_sem.at[0])
    keep.start()

    def report(step, who):
        pltpu.make_async_remote_copy(
            src_ref=stat,
            dst_ref=inbox.at[step - 1],
            send_sem=stat_send,
            recv_sem=stat_recv,
            device_id=who,
            device_id_type=MESH,
        ).start()

    each_peer(report, outward=False)
    pltpu.make_async_copy(inbox, inbox, stat_recv).wait()
    sums = stat[...] + jnp.sum(inbox[...], axis=0)
    mean_sq = jnp.sum(sums[0:1], axis=1, keepdims=True) / jnp.sum(sums[1:2], axis=1, keepdims=True)
    tension[...] = squared[...] / (mean_sq + 1e-06)
    last = pltpu.make_async_copy(tension, tension_hbm, end_sem.at[1])
    last.start()
    pltpu.make_async_copy(inbox, inbox, stat_send).wait()
    keep.wait()
    last.wait()


def hand_over(drift_in, tension_in, drift_out, tension_out, drift_mid, tension_mid, sems):
    ways = ((drift_in, drift_mid, drift_out), (tension_in, tension_mid, tension_out))
    came = [pltpu.make_async_copy(src, mid, sems.at[i]) for i, (src, mid, _) in enumerate(ways)]
    gone = [pltpu.make_async_copy(mid, dst, sems.at[2 + i]) for i, (_, mid, dst) in enumerate(ways)]
    for copy in came:
        copy.start()
    for copy, onward in zip(came, gone):
        copy.wait()
        onward.start()
    for onward in gone:
        onward.wait()


def shards(positions_now, velocities, positions_next, halo_counts, neighbour_lists, descendants):
    slots = positions_now.shape[-1]
    cx, cy, cz, width = neighbour_lists.shape
    cells = cx * cy * cz
    sizes = tuple(lax.axis_size(name) for name in AXES)
    folded = sizes[2] == 2 and cz == 1
    planes = 2 if folded else cz + 2
    padded = (cx + 2) * (cy + 2) * (cz + 2)
    ways = 17 if folded else 26
    peers = sizes[0] * sizes[1] * sizes[2] - 1

    def rows(array):
        return jnp.transpose(array, (0, 1, 2, 3, 4)).reshape(cells * 3, slots)

    ends, tension = pl.pallas_call(
        functools.partial(kernel, (cx, cy, cz), width, sizes),
        out_shape=(
            jax.ShapeDtypeStruct((cells * 3, slots), jnp.float32),
            jax.ShapeDtypeStruct((cells, slots), jnp.float32),
        ),
        in_specs=[pl.BlockSpec(memory_space=pl.ANY)] * 6,
        out_specs=(pl.BlockSpec(memory_space=pl.ANY),) * 2,
        scratch_shapes=[
            pltpu.SMEM((cells, 1, width), jnp.int32),
            pltpu.SMEM((cy, cz, cx), jnp.int32),
            pltpu.VMEM((cells, 4, slots), jnp.float32),
            pltpu.VMEM((cells * 3, slots), jnp.float32),
            pltpu.VMEM((cells * 3, slots), jnp.float32),
            pltpu.VMEM((cells, 2, slots), jnp.int32),
            pltpu.VMEM((cx + 2, cy + 2, planes, 4, slots), jnp.float32),
            pltpu.VMEM((cx + 2, cy + 2, planes, 4, slots), jnp.float32),
            pltpu.VMEM((padded, slots, slots), jnp.bfloat16),
            pltpu.VMEM((padded, 16, slots), jnp.bfloat16),
            pltpu.VMEM((cells, ROWS, slots), jnp.bfloat16),
            pltpu.VMEM((cells * 3, slots), jnp.float32),
            pltpu.VMEM((cells, slots), jnp.float32),
            pltpu.VMEM((cells, slots), jnp.float32),
            pltpu.VMEM((2, slots), jnp.float32),
            pltpu.VMEM((peers, 2, slots), jnp.float32),
            pltpu.SemaphoreType.DMA((6,)),
            pltpu.SemaphoreType.DMA((2,)),
            pltpu.SemaphoreType.DMA((ways,)),
            pltpu.SemaphoreType.DMA((ways,)),
            pltpu.SemaphoreType.DMA((ways,)),
            pltpu.SemaphoreType.DMA((ways,)),
            pltpu.SemaphoreType.DMA,
            pltpu.SemaphoreType.DMA,
        ],
        compiler_params=pltpu.CompilerParams(collective_id=0, has_side_effects=True),
    )(
        neighbour_lists.reshape(cells, 1, width),
        jnp.transpose(halo_counts, (1, 2, 0)),
        positions_now.reshape(cells, 4, slots),
        rows(positions_next),
        rows(velocities),
        descendants.reshape(cells, 2, slots),
    )
    drift, tension = pl.pallas_call(
        hand_over,
        out_shape=(
            jax.ShapeDtypeStruct((cells * 3, slots), jnp.float32),
            jax.ShapeDtypeStruct((cells, slots), jnp.float32),
        ),
        in_specs=[pl.BlockSpec(memory_space=pl.ANY)] * 2,
        out_specs=(pl.BlockSpec(memory_space=pl.ANY),) * 2,
        scratch_shapes=[
            pltpu.VMEM((cells * 3, slots), jnp.float32),
            pltpu.VMEM((cells, slots), jnp.float32),
            pltpu.SemaphoreType.DMA((4,)),
        ],
    )(ends, tension)
    return (drift.reshape(cx, cy, cz, 3, slots), tension.reshape(cx, cy, cz, slots))


def solution(mesh):
    return jax.shard_map(
        shards,
        mesh=mesh,
        in_specs=(
            P("gx", "gy", "gz", None, None),
            P("gx", "gy", "gz", None, None),
            P("gx", "gy", "gz", None, None),
            P("gx", "gy", "gz"),
            P("gx", "gy", "gz", None),
            P("gx", "gy", "gz", None, None),
        ),
        out_specs=(P("gx", "gy", "gz", None, None), P("gx", "gy", "gz", None)),
        check_vma=False,
    )
```
